128 devices in a mesh: dp: 16 (over z, x), expert: 8 (over y, core).
Axes of the slice: x: 4, y: 4, z: 4, core: 2. Of those that a mesh axis runs over, the one named last changes fastest.
Arguments:
- tokens: bfloat16 [16384, 2048], P(('dp', 'expert')), may hold values from -6 to 6
- cotangent: bfloat16 [16384, 2048], P(('dp', 'expert')), may hold values from -6 to 6
- expert_ids: int32 [16384, 2], P(('dp', 'expert')), may hold values from 0 to 7, all different within a row; in each aligned block of 128 rows (0 to 127, 128 to 255, ...) at most 36 rows name the same one
- route_share: float32 [16384], P(('dp', 'expert')), may hold values from 0.5 to 0.95
- gate_proj: bfloat16 [8, 7168, 2048], P('expert', 'dp'), may hold values from -0.125 to 0.125
- up_proj: bfloat16 [8, 7168, 2048], P('expert', 'dp'), may hold values from -0.125 to 0.125
- down_anchor: float32 [8, 7168, 2048], P('expert', 'dp'), may hold values from -0.12 to 0.12
- down_average: float32 [8, 7168, 2048], P('expert', 'dp'), may hold values from -0.12 to 0.12
- down_moment: float32 [8, 7168, 2048], P('expert', 'dp'), may hold values from 0.002 to 0.05
Outputs:
- new_anchor: float32 [8, 7168, 2048], P('expert', 'dp')
- new_average: float32 [8, 7168, 2048], P('expert', 'dp')
- new_moment: float32 [8, 7168, 2048], P('expert', 'dp')
The draws below stay inside these ranges and needn't reach their ends.
Inputs may be any that keep to these rules, and one draw needn't show every extreme that they name: `expert_ids`: the two ids of a token differ. The rows of one device name any expert at most 36 times, and in every draw some device names some expert exactly 36 times.
All inputs are finite; a program needn't handle non-finite values.
Results may differ from the reference program's by a relative error of at most 0.0043.
Values may be sent and summed in bfloat16 or wider, within the bound.
No kernel may reach another device: no remote copies, remote signals or barrier semaphores. Data moves between devices by JAX's collectives and lax.ppermute only.
A program may use at most 192 MiB of HBM per device.

```python
import math
import jax
import jax.numpy as jnp
import numpy as np
from jax import lax

D = 2048
FF = 7168
TOPK = 2
TOK_DEV = 128
EXPERTS = 8
CAP = 36
TOKENS = 16384
DEVICES = 128


def shard_levels(rng, extent, pieces, least, top_value):
    def one(position, blocks):
        draws = jax.random.uniform(jax.random.fold_in(jax.random.fold_in(rng, 6), position), (blocks,), jnp.float32, least / len(pieces), top_value / len(pieces))
        return jnp.repeat(jnp.exp(draws), extent[position] // blocks).reshape((-1,) + (1,) * (len(extent) - position - 1))

    gain = one(*pieces[0])
    for cut in pieces[1:]:
        gain = gain * one(*cut)
    return gain


def routed_block(key, own, number, rows, number_of, top, most, skew):
    order = jax.random.permutation(key, number_of)
    crowded, common = portions_of(number_of, rows * top, most, skew, True), portions_of(number_of, rows * top, most, skew, False)
    places = jnp.arange(number_of)

    def named(sizes, rotation):
        used = int((sizes > 0).sum())
        fixed = max(1, used // 4)
        passed = fixed + (places - fixed + rotation * (used - fixed)) % max(1, number_of - fixed)
        return jnp.zeros((number_of,), jnp.int32).at[order[jnp.where(places < fixed, places, passed)]].set(jnp.asarray(sizes, jnp.int32))

    sizes = jnp.where(number % 4 == 0, named(crowded, number // 4), named(common, number - number // 4 - 1))
    mixed = jax.random.permutation(jax.random.fold_in(own, 3), number_of)
    donor, sink = mixed[0:number_of // 2 * 2:2], mixed[1:number_of // 2 * 2:2]
    margin = jnp.minimum(sizes[donor] - 1, most - sizes[sink]) // 2
    margin = jnp.where((donor == order[0]) | (sink == order[0]) | (sizes[sink] == 0), 0, jnp.maximum(margin, 0))
    passed = jax.random.randint(jax.random.fold_in(own, 4), (number_of // 2,), 0, 1 << 20) % (margin + 1)
    sizes = sizes.at[donor].add(-passed).at[sink].add(passed)
    members = jnp.searchsorted(jnp.cumsum(sizes), jnp.arange(rows * top), side="right").astype(jnp.int32)
    listing = members.reshape(top, rows).T
    listing = listing[jax.random.permutation(jax.random.fold_in(own, 1), rows)]
    rotation = jax.random.randint(jax.random.fold_in(own, 2), (rows, 1), 0, top)
    return jnp.take_along_axis(listing, (jnp.arange(top)[None, :] + rotation) % top, axis=1)


def portions_of(number_of, total, limit, skew, full):
    portions = [(1 << 20) // math.isqrt(rank ** skew) + 1 for rank in range(1, number_of + 1)]
    largest = limit if full else min(limit, max(-(-total // number_of), total * portions[0] // sum(portions)))
    least = 1 if total - largest >= number_of - 1 else 0
    holding, surplus = [largest] + [least] * (number_of - 1), total - largest - least * (number_of - 1)
    while surplus > 0:
        candidates = [i for i in range(1, number_of) if holding[i] < largest] or [i for i in range(1, number_of) if holding[i] < limit]
        pool, left = sum([portions[i] for i in candidates]), surplus
        for i in candidates:
            extra = min(limit - holding[i], max(1, left * portions[i] // pool), surplus)
            holding[i] = holding[i] + extra
            surplus = surplus - extra
    return np.array(holding)


def noise(stream_key, shape, spread, reach, split=(), kind=jnp.bfloat16):
    entries = jax.random.normal(stream_key, shape, jnp.float32) * spread
    if len(split) > 0:
        entries = shard_levels(stream_key, shape, split, -0.22, 0.18) * entries
    return jnp.clip(entries, min=-reach, max=reach).astype(kind)


def setup_inputs(seed: int = 0) -> dict:
    streams_of = jax.random.split(jax.random.key(seed), 10)
    tokens = noise(streams_of[0], (TOKENS, D), 1.0, 6.0, ((0, 128),))
    cotangent = noise(streams_of[1], (TOKENS, D), 1.0, 6.0, ((0, 128),))
    expert_ids_keys = jax.random.split(jax.random.fold_in(streams_of[2], 1), TOKENS // TOK_DEV)
    expert_ids_turns = jax.random.permutation(jax.random.fold_in(streams_of[2], 3), TOKENS // TOK_DEV)
    expert_ids = jax.vmap(lambda own, number: routed_block(jax.random.fold_in(streams_of[2], 2), own, number, TOK_DEV, EXPERTS, TOPK, CAP, 1))(expert_ids_keys, expert_ids_turns).reshape((TOKENS, TOPK))
    route_share = jnp.clip(0.5 + 0.45 * jax.random.uniform(streams_of[3], (TOKENS,), jnp.float32) ** shard_levels(streams_of[3], (TOKENS,), ((0, 128),), -0.2, 0.2), 0.5, 0.95)
    gate_proj = noise(streams_of[4], (EXPERTS, FF, D), D ** -0.5, 0.125, ((0, 8), (1, 16)))
    up_proj = noise(streams_of[5], (EXPERTS, FF, D), D ** -0.5, 0.125, ((0, 8), (1, 16)))
    down_anchor = noise(streams_of[6], (EXPERTS, FF, D), 0.02, 0.12, ((0, 8), (1, 16)), jnp.float32)
    down_average = noise(streams_of[7], (EXPERTS, FF, D), 0.02, 0.12, ((0, 8), (1, 16)), jnp.float32)
    down_moment = jnp.clip(jnp.exp(math.log(0.05) - 3.218876 * jax.random.uniform(streams_of[8], (EXPERTS, FF, D), jnp.float32) ** shard_levels(streams_of[8], (EXPERTS, FF, D), ((0, 8), (1, 16)), -0.2, 0.2)), 0.002, 0.05)
    return {"tokens": tokens, "cotangent": cotangent, "expert_ids": expert_ids, "route_share": route_share, "gate_proj": gate_proj, "up_proj": up_proj, "down_anchor": down_anchor, "down_average": down_average, "down_moment": down_moment}


beta_one = 0.9
beta_two = 0.95
learn_rate = 0.05
decay_rate = 0.1
step_count = 4.0
epsilon = 1e-08

def reference(tokens, cotangent, expert_ids, route_share, gate_proj, up_proj, down_anchor, down_average, down_moment):
    shares = jnp.stack([route_share, 1.0 - route_share], axis=1)
    flat_ids = expert_ids.reshape(-1).astype(jnp.int32)
    flat_tok = (jnp.arange(TOKENS * TOPK, dtype=jnp.int32) // TOPK).astype(jnp.int32)
    flat_share = shares.reshape(-1)
    by_expert = jnp.argsort(flat_ids, stable=True).astype(jnp.int32)
    sorted_tok = flat_tok[by_expert]
    gated = (flat_share[by_expert][:, None] * cotangent[sorted_tok].astype(jnp.float32)).astype(jnp.bfloat16)
    rows_in = tokens[sorted_tok]
    expert_range = jnp.arange(EXPERTS, dtype=jnp.int32)
    counts = lax.optimization_barrier(jnp.sum((flat_ids[:, None] == expert_range[None, :]).astype(jnp.int32), axis=0)).astype(jnp.int32)
    starts = (jnp.cumsum(counts) - counts).astype(jnp.int32)
    window = DEVICES * CAP
    pad_rows = jnp.zeros((window, D), jnp.bfloat16)
    rows_in = jnp.concatenate([rows_in, pad_rows], 0)
    gated = jnp.concatenate([gated, pad_rows], 0)

    def one_expert(expert_number):
        begin_row = starts[expert_number]
        xrows = lax.dynamic_slice_in_dim(rows_in, begin_row, window, 0)
        drows = lax.dynamic_slice_in_dim(gated, begin_row, window, 0)
        live_rows = jnp.arange(window, dtype=jnp.int32) < counts[expert_number]
        drows = jnp.where(live_rows[:, None], drows, jnp.zeros_like(drows))
        gate_rows = lax.dynamic_index_in_dim(gate_proj, expert_number, 0, keepdims=False)
        up_rows = lax.dynamic_index_in_dim(up_proj, expert_number, 0, keepdims=False)
        gate_act = jnp.dot(xrows, gate_rows.T, preferred_element_type=jnp.float32)
        up_act = jnp.dot(xrows, up_rows.T, preferred_element_type=jnp.float32)
        hidden = (jax.nn.silu(gate_act) * up_act).astype(jnp.bfloat16)
        return jnp.dot(hidden.T, drows, preferred_element_type=jnp.float32)
    gradient = lax.map(one_expert, expert_range) * FF ** (-0.5)
    bias_two = 1.0 - beta_two ** step_count
    eval_point = (1.0 - beta_one) * down_anchor + beta_one * down_average
    second_moment = beta_two * down_moment + (1.0 - beta_two) * gradient * gradient
    update_dir = gradient / (jnp.sqrt(second_moment / bias_two) + epsilon) + decay_rate * eval_point
    new_anchor = down_anchor - learn_rate * update_dir
    new_average = (1.0 - 1.0 / step_count) * down_average + 1.0 / step_count * new_anchor
    return (new_anchor, new_average, second_moment)
```

```python
import jax
import jax.numpy as jnp
from jax import lax
from jax.sharding import PartitionSpec as P

FF = 7168
TOPK = 2
NX = 4
NZ = 4
NY = 4


beta_one = 0.9
beta_two = 0.95
learn_rate = 0.05
decay_rate = 0.1
step_count = 4.0
epsilon = 1e-08

T_COLS = ((0, 1152), (1152, 2048))
D_COLS = ((0, 640), (640, 1152), (1152, 1664), (1664, 2048))


def dp_pairs(move):
    pairs = []
    for z in range(NZ):
        for x in range(NX):
            nz, nx = move(z, x)
            pairs.append((z * NX + x, (nz % NZ) * NX + nx % NX))
    return pairs


Z_UP = dp_pairs(lambda z, x: (z + 1, x))
Z_DOWN = dp_pairs(lambda z, x: (z - 1, x))
X_ROW = dp_pairs(lambda z, x: (z, 3 - x))
X_WEIGHT = dp_pairs(lambda z, x: (z, x ^ 1))
CORE = [(e, e ^ 1) for e in range(2 * NY)]


def y_pairs(offset):
    return [(e, (e + 2 * offset) % (2 * NY)) for e in range(2 * NY)]


def gather_x_then_z(v):
    b = lax.ppermute(v, "dp", X_ROW)
    v_below = lax.ppermute(v, "dp", Z_UP)
    v_above = lax.ppermute(v, "dp", Z_DOWN)
    b_below = lax.ppermute(b, "dp", Z_UP)
    b_above = lax.ppermute(b, "dp", Z_DOWN)
    v_far = lax.ppermute(v_below, "dp", Z_UP)
    b_far = lax.ppermute(b_above, "dp", Z_DOWN)
    return [v, b, v_below, b_below, v_above, b_above, v_far, b_far]


def gather_z_then_x(v):
    half = v.shape[0] // 2
    below = lax.ppermute(v, "dp", Z_UP)
    above = lax.ppermute(v, "dp", Z_DOWN)
    b = lax.ppermute(v, "dp", X_ROW)
    far_a = lax.ppermute(below[:half], "dp", Z_UP)
    far_b = lax.ppermute(above[half:], "dp", Z_DOWN)
    far = jnp.concatenate([far_a, far_b], axis=0)
    b_below = lax.ppermute(below, "dp", X_ROW)
    b_above = lax.ppermute(above, "dp", X_ROW)
    b_far = lax.ppermute(far, "dp", X_ROW)
    return [v, b, below, b_below, above, b_above, far, b_far]


def hidden_of(rows, weight_gate, weight_up):
    dims = (((1,), (1,)), ((), ()))
    gate_act = lax.dot_general(rows, weight_gate, dims, preferred_element_type=jnp.float32)
    up_act = lax.dot_general(rows, weight_up, dims, preferred_element_type=jnp.float32)
    return (jax.nn.silu(gate_act) * up_act).astype(jnp.bfloat16)


def contract_rows(hidden, rows):
    return lax.dot_general(
        hidden, rows, (((0,), (0,)), ((), ())), preferred_element_type=jnp.float32
    )


def shards(
    tokens,
    cotangent,
    expert_ids,
    route_share,
    gate_proj,
    up_proj,
    down_anchor,
    down_average,
    down_moment,
):
    tok_rows = tokens.shape[0]
    width = tokens.shape[1]
    capacity = 36
    weight_gate = gate_proj[0]
    weight_up = up_proj[0]
    gate_far = lax.ppermute(weight_gate, "dp", X_WEIGHT)
    up_far = lax.ppermute(weight_up, "dp", X_WEIGHT)

    ids_far = lax.ppermute(expert_ids, "expert", CORE)
    share_far = lax.ppermute(route_share, "expert", CORE)
    tok_far = lax.ppermute(tokens, "expert", CORE)
    cot_far = lax.ppermute(cotangent, "expert", CORE)
    me = lax.axis_index("expert")
    my_core = me % 2
    my_y = me // 2

    def target_of(ids, first):
        expert_range = jnp.arange(2 * NY, dtype=jnp.int32)
        flat = ids.reshape(-1)
        onehot = (flat[:, None] == expert_range[None, :]).astype(jnp.int32)
        earlier = jnp.cumsum(onehot, axis=0) - onehot
        rank = jnp.sum(earlier * onehot, axis=1)
        block = (flat // 2 - my_y + NY) % NY
        slot = block * (2 * capacity) + first + rank
        return jnp.where(flat % 2 == my_core, slot, -1).reshape(tok_rows, TOPK)

    target = jnp.concatenate([target_of(expert_ids, 0), target_of(ids_far, capacity)], axis=0)
    share = jnp.concatenate([route_share, share_far], axis=0)
    shares = jnp.stack([share, 1.0 - share], axis=1)
    slots = 2 * NY * capacity
    slot_range = jnp.arange(slots, dtype=jnp.int32)
    placed = target[None, :, :] == slot_range[:, None, None]
    picker = jnp.sum(placed.astype(jnp.float32), axis=2).astype(jnp.bfloat16)
    slot_share = jnp.sum(jnp.where(placed, shares[None, :, :], 0.0), axis=(1, 2))
    chip_tok = jnp.concatenate([tokens, tok_far], axis=0)
    chip_cot = jnp.concatenate([cotangent, cot_far], axis=0)
    pick_tok = jnp.dot(picker, chip_tok, preferred_element_type=jnp.float32).astype(jnp.bfloat16)
    pick_cot = (
        slot_share[:, None] * jnp.dot(picker, chip_cot, preferred_element_type=jnp.float32)
    ).astype(jnp.bfloat16)

    def over_y(picked):
        step = 2 * capacity
        blocks = [picked[:step]]
        for k in range(1, NY):
            blocks.append(lax.ppermute(picked[k * step : (k + 1) * step], "expert", y_pairs(k)))
        return blocks

    tok_blocks = over_y(pick_tok)
    cot_blocks = over_y(pick_cot)

    def own_piece(blocks, cols):
        return jnp.concatenate([block[:, cols[0] : cols[1]] for block in blocks], axis=0)

    def gathered(blocks, cols, number):
        gather = gather_x_then_z if number % 2 == 0 else gather_z_then_x
        return gather(own_piece(blocks, cols))

    tok_parts = [gathered(tok_blocks, cols, n) for n, cols in enumerate(T_COLS)]
    rows_in = jnp.concatenate(
        [jnp.concatenate([part[i] for part in tok_parts], axis=1) for i in range(8)], axis=0
    )
    hidden_own = hidden_of(rows_in, weight_gate, weight_up)
    hidden_far = hidden_of(rows_in, gate_far, up_far)

    bias_two = 1.0 - beta_two**step_count
    scale = FF ** (-0.5)
    outs = []
    for n, cols in enumerate(D_COLS):
        rows = jnp.concatenate(gathered(cot_blocks, cols, n), axis=0)
        partial_far = contract_rows(hidden_far, rows).astype(jnp.bfloat16)
        partial_here = lax.ppermute(partial_far, "dp", X_WEIGHT)
        gradient = (contract_rows(hidden_own, rows) + partial_here.astype(jnp.float32)) * scale
        anchor = down_anchor[0, :, cols[0] : cols[1]]
        average = down_average[0, :, cols[0] : cols[1]]
        moment = down_moment[0, :, cols[0] : cols[1]]
        eval_point = (1.0 - beta_one) * anchor + beta_one * average
        second = beta_two * moment + (1.0 - beta_two) * gradient * gradient
        update = gradient / (jnp.sqrt(second / bias_two) + epsilon) + decay_rate * eval_point
        new_anchor = anchor - learn_rate * update
        new_average = (1.0 - 1.0 / step_count) * average + 1.0 / step_count * new_anchor
        outs.append((new_anchor, new_average, second))
    return tuple(jnp.concatenate([o[i] for o in outs], axis=1)[None] for i in range(3))


def solution(mesh):
    rows = P(("dp", "expert"), None)
    state = P("expert", "dp", None)
    return jax.shard_map(
        shards,
        mesh=mesh,
        in_specs=(rows, rows, rows, P(("dp", "expert")), state, state, state, state, state),
        out_specs=(state, state, state),
        check_vma=False,
    )
```
